256 devices in a mesh: parts: 4 (over x, y), env: 64 (over z, core).
Axes of the slice: x: 2, y: 2, z: 32, core: 2. Of those that a mesh axis runs over, the one named last changes fastest.
The devices are a block of a 4x8x32 slice.
Arguments:
- first_obs: float32 [48, 32768], P(None, ('parts', 'env')), parts along dimension 1, may hold values from -6 to 6
- dyn_state: float32 [48, 48], replicated, may hold values from -0.875 to 0.875
- dyn_act: float32 [48, 12], replicated, may hold values from -1.75 to 1.75
- contact_gain: float32 [4, 48, 48], replicated, may hold values from -0.875 to 0.875
- reward_weight: float32 [48], replicated, may hold values from 0.1 to 1
- contacts: int32 [8, 4, 32768], P(None, None, ('parts', 'env')), parts along dimension 2, may hold values 0 or 1
- action_noise: int32 [8, 12, 32768], P(None, None, ('parts', 'env')), parts along dimension 2, may hold values from -32768 to 32767
- policy_in: bfloat16 [512, 48], replicated, may hold values from -0.875 to 0.875
- policy_out: bfloat16 [12, 512], replicated, may hold values from -0.25 to 0.25
- critic_in: bfloat16 [48, 1024], replicated, may hold values from -0.875 to 0.875
- critic_middle: bfloat16 [1024, 1024], replicated, may hold values from -0.1875 to 0.1875
- critic_out: bfloat16 [1024], replicated, may hold values from -0.1875 to 0.1875
Outputs:
- td_targets: float32 [8, 32768], P(None, ('parts', 'env')), parts along dimension 1
- grad_middle: float32 [4096, 1024], P(('parts', 'env')), parts along dimension 0
- grad_in: float32 [192, 1024], P('parts'), parts along dimension 0
- grad_out: float32 [4096], P('parts'), parts along dimension 0
The draws below stay inside these ranges and needn't reach their ends.
There are 4 independent parts, one for each index of `parts`. The reference program is written for one: setup_inputs(seed, part) draws one part's arguments, and reference() takes and returns one part's arrays. A program takes and returns all parts, laid end to end along the dimension named above; an argument that names none is the same for every part. Nothing has to cross between parts.
Inputs may be any that keep to these rules, and one draw needn't show every extreme that they name: `contacts`: 1 where the foot is in contact. `action_noise`: noise in units of 0.3 / 32768.
All inputs are finite; a program needn't handle non-finite values. No bound on the sum of `contacts` on one device may be relied on, other than what follows from the above.
Results may differ from the reference program's by a relative error of at most 0.018.
Values sent between devices are 32-bit elements; how exact they have to be, the bound alone decides.
No kernel may reach another device: no remote copies, remote signals or barrier semaphores. Data moves between devices by JAX's collectives and lax.ppermute only.
A program may use at most 64 MiB of HBM per device.

```python
import math
import jax
import jax.numpy as jnp
from jax import lax

OBS = 48
ACT = 12
FEET = 4
POL_H = 512
H = 1024
STEPS = 8
ENV_DEV = 128
ENVS = 8192


def set_ends(result, key, smallest, top_value):
    longest = result.shape.index(max(result.shape))
    spots = []
    for shift in (0, 1):
        where = [jax.random.randint(jax.random.fold_in(key, axis), (), 0, length) for axis, length in enumerate(result.shape)]
        where[longest] = (where[longest] + shift) % result.shape[longest]
        spots.append(tuple(where))
    return result.at[spots[0]].set(smallest).at[spots[1]].set(top_value)


def levels(rng, shape, split, low, top_value):
    def one(dim, blocks):
        steps = jax.random.uniform(jax.random.fold_in(jax.random.fold_in(rng, 6), dim), (blocks,), jnp.float32, low / len(split), top_value / len(split))
        return jnp.repeat(jnp.exp(steps), shape[dim] // blocks).reshape((-1,) + (1,) * (len(shape) - dim - 1))

    gain = one(*split[0])
    for cut in split[1:]:
        gain = gain * one(*cut)
    return gain


def centred(own_key, shape, deviation, bound, split=(), held_as=jnp.bfloat16):
    level = levels(own_key, shape, split, -0.22, 0.18) if split else 1.0
    drawn = jax.random.normal(own_key, shape, jnp.float32) * deviation * level
    return jnp.minimum(jnp.maximum(drawn, -bound), bound).astype(held_as)


def setup_inputs(seed: int = 0, part: int = 0) -> dict:
    streams_of = jax.random.split(jax.random.key(seed), 13)
    own_keys = jax.random.split(jax.random.fold_in(streams_of[12], part), 13)
    first_obs = centred(own_keys[0], (OBS, ENVS), 1.0, 6.0, ((1, 64),), jnp.float32)
    dyn_state = centred(streams_of[1], (OBS, OBS), OBS ** -0.5, 0.875, (), jnp.float32)
    dyn_act = centred(streams_of[2], (OBS, ACT), ACT ** -0.5, 1.75, (), jnp.float32)
    contact_gain = centred(streams_of[3], (FEET, OBS, OBS), OBS ** -0.5, 0.875, (), jnp.float32)
    reward_weight = jnp.clip(jnp.exp(jax.random.uniform(streams_of[4], (OBS,), jnp.float32, math.log(0.1), math.log(1.0))), 0.1, 1.0)
    contacts = set_ends((jax.random.randint(own_keys[5], (STEPS, FEET, ENVS), 0, 2) < 1).astype(jnp.int32), jax.random.fold_in(own_keys[5], 1), 0, 1)
    action_noise = set_ends(jax.random.randint(own_keys[6], (STEPS, ACT, ENVS), -32768, 32768), jax.random.fold_in(own_keys[6], 1), -32768, 32767).astype(jnp.int32)
    policy_in = centred(streams_of[7], (POL_H, OBS), OBS ** -0.5, 0.875)
    policy_out = centred(streams_of[8], (ACT, POL_H), POL_H ** -0.5, 0.25)
    critic_in = centred(streams_of[9], (OBS, H), OBS ** -0.5, 0.875)
    critic_middle = centred(streams_of[10], (H, H), H ** -0.5, 0.1875)
    critic_out = centred(streams_of[11], (H,), H ** -0.5, 0.1875)
    return dict(first_obs=first_obs, dyn_state=dyn_state, dyn_act=dyn_act, contact_gain=contact_gain, reward_weight=reward_weight, contacts=contacts, action_noise=action_noise, policy_in=policy_in, policy_out=policy_out, critic_in=critic_in, critic_middle=critic_middle, critic_out=critic_out)


time_step = 0.05
noise_unit = 0.3 / 32768.0
discount = 0.99
trace_decay = 0.95

def rollout(first_obs, dyn_state, dyn_act, contact_gain, reward_weight, contacts, action_noise, policy_in, policy_out):
    highest = lax.Precision.HIGHEST
    state_now = first_obs
    states = [state_now]
    rewards = []
    for step in range(contacts.shape[0]):
        hidden = jnp.tanh(jnp.dot(policy_in, state_now, precision=highest))
        action = jnp.tanh(jnp.dot(policy_out, hidden, precision=highest)) + noise_unit * action_noise[step].astype(jnp.float32)
        pushed = jnp.einsum('kij,je->kie', contact_gain, state_now, precision=highest)
        contact_force = lax.optimization_barrier(jnp.sum(pushed * contacts[step].astype(jnp.float32)[:, None, :], axis=0))
        drift_rate = jnp.tanh(jnp.dot(dyn_state, state_now, precision=highest)) + jnp.dot(dyn_act, action, precision=highest) - contact_force
        state_next = state_now + time_step * drift_rate
        reward = 0.5 - lax.optimization_barrier(jnp.mean(reward_weight[:, None] * state_next * state_next, axis=0)) - 0.1 * lax.optimization_barrier(jnp.mean(action * action, axis=0))
        states.append(state_next)
        rewards.append(reward)
        state_now = state_next
    return (jnp.stack(states), jnp.stack(rewards))

def critic_block(states, rewards, critic_in, critic_out, forward_middle, backward_middle, loss_scale):
    state_count, obs_dim, env_count = states.shape
    inputs = jnp.transpose(states, (0, 2, 1)).reshape(-1, obs_dim).astype(jnp.bfloat16)
    first_pre = jnp.dot(inputs, critic_in, preferred_element_type=jnp.float32)
    first_act = jnp.maximum(first_pre, 0.0).astype(jnp.bfloat16)
    middle_pre = forward_middle(first_act)
    middle_act = jnp.maximum(middle_pre, 0.0).astype(jnp.bfloat16)
    values = jnp.dot(middle_act, critic_out, preferred_element_type=jnp.float32).reshape(state_count, env_count)
    target = values[state_count - 1]
    backward_rows = []
    for step in reversed(range(state_count - 1)):
        target = rewards[step] + discount * ((1.0 - trace_decay) * values[step + 1] + trace_decay * target)
        backward_rows.append(target)
    targets = jnp.stack(backward_rows[::-1])
    errors = values[:-1] - targets
    row_weight = jnp.concatenate([loss_scale * errors, jnp.zeros((1, env_count), jnp.float32)], axis=0).reshape(-1)
    grad_out = lax.optimization_barrier(jnp.sum(row_weight[:, None] * middle_act.astype(jnp.float32), axis=0))
    middle_delta = jnp.where(middle_pre > 0, row_weight[:, None] * critic_out.astype(jnp.float32)[None, :], 0.0).astype(jnp.bfloat16)
    first_back = backward_middle(middle_delta)
    first_delta = jnp.where(first_pre > 0, first_back, 0.0).astype(jnp.bfloat16)
    grad_in = lax.dot_general(inputs, first_delta, (((0,), (0,)), ((), ())), preferred_element_type=jnp.float32)
    return (targets, first_act, middle_delta, grad_in, grad_out)

def reference(first_obs, dyn_state, dyn_act, contact_gain, reward_weight, contacts, action_noise, policy_in, policy_out, critic_in, critic_middle, critic_out):
    states, rewards = rollout(first_obs, dyn_state, dyn_act, contact_gain, reward_weight, contacts, action_noise, policy_in.astype(jnp.float32), policy_out.astype(jnp.float32))
    blocks = ENVS // ENV_DEV
    state_blocks = states.reshape(STEPS + 1, OBS, blocks, ENV_DEV).transpose(2, 0, 1, 3)
    reward_blocks = rewards.reshape(STEPS, blocks, ENV_DEV).transpose(1, 0, 2)
    loss_scale = math.sqrt(H) / (STEPS * ENVS)

    def forward_middle(first_act):
        return jnp.dot(first_act, critic_middle, preferred_element_type=jnp.float32)

    def backward_middle(middle_delta):
        return lax.dot_general(middle_delta, critic_middle, (((1,), (1,)), ((), ())), preferred_element_type=jnp.float32)

    def one_block(totals, block):
        targets, first_act, middle_delta, grad_in, grad_out = critic_block(block[0], block[1], critic_in, critic_out, forward_middle, backward_middle, loss_scale)
        grad_mid = lax.dot_general(first_act, middle_delta, (((0,), (0,)), ((), ())), preferred_element_type=jnp.float32)
        return ((totals[0] + grad_mid, totals[1] + grad_in, totals[2] + grad_out), targets)
    initial = (jnp.zeros((H, H), jnp.float32), jnp.zeros((OBS, H), jnp.float32), jnp.zeros((H,), jnp.float32))
    totals, target_blocks = lax.scan(one_block, initial, (state_blocks, reward_blocks))
    td_targets = target_blocks.transpose(1, 0, 2).reshape(STEPS, ENVS)
    return (td_targets, totals[0], totals[1], totals[2])
```

```python
import functools
import math

import jax
import jax.numpy as jnp
import numpy as np
from jax import lax
from jax.experimental import pallas as pl
from jax.experimental.pallas import tpu as pltpu
from jax.sharding import PartitionSpec as P

TIME_STEP = 0.05
NOISE_UNIT = 0.3 / 32768.0
DISCOUNT = 0.99
TRACE_DECAY = 0.95
LEVELS = 2
CORES = 2

F32 = jnp.float32
BF16 = jnp.bfloat16
NT = (((1,), (1,)), ((), ()))
TN = (((0,), (0,)), ((), ()))


def mm(a, b, dims=(((1,), (0,)), ((), ()))):
    return lax.dot_general(a, b, dims, preferred_element_type=F32)


def message_orders(ring):
    d = 2**LEVELS
    half = ring // 2
    behind = [-o for o in range(d, half + 1, d)]
    ahead = list(range(half, 0, -d))
    orders = [behind[:-1] + ahead + [0]]
    for level in reversed(range(LEVELS)):
        d = 2**level
        right, left = [o + d for o in behind], [o - d for o in ahead]
        orders = [right, left] + orders
        behind, ahead = right + behind, left + ahead
    return orders


def column(row, lanes):
    return jnp.transpose(jnp.broadcast_to(row, (lanes, row.shape[1])))


def window_kernel(
    loss_scale,
    sizes,
    slot_ref,
    obs_ref,
    dyn_state_ref,
    dyn_act_ref,
    gain_ref,
    reward_weight_ref,
    contacts_ref,
    noise_ref,
    policy_in_ref,
    policy_out_ref,
    critic_in_ref,
    critic_middle_ref,
    critic_out_ref,
    targets_ref,
    small_ref,
    grad_ref,
    state_mix,
    inputs,
    first,
    middle,
    delta,
    first_delta,
    middle_t,
    out_col,
    act_cols,
    weight_col,
):
    obs, env = obs_ref.shape
    steps, feet, _ = contacts_ref.shape
    act = dyn_act_ref.shape[0]
    pol = policy_out_ref.shape[1]
    hid = critic_middle_ref.shape[0]
    rows = steps * env
    cores, ring, depth = CORES, sum(sizes), grad_ref.shape[2]
    index = lax.axis_index("env")
    here, core = index // cores, lax.rem(index, cores)

    mixing = jnp.concatenate(
        [jnp.transpose(policy_in_ref[...].astype(F32)), dyn_state_ref[...]]
        + [gain_ref[k] for k in range(feet)],
        axis=0,
    )
    top = mixing.astype(BF16).astype(F32)
    state_mix[...] = jnp.concatenate([top, top, mixing - top], axis=1).astype(BF16)
    for a in range(act):
        act_cols[a] = column(dyn_act_ref[a : a + 1, :], env)
    weight_col[...] = column(reward_weight_ref[...], env)
    out_col[...] = column(critic_out_ref[...].astype(F32), env)
    middle_t[...] = jnp.transpose(critic_middle_ref[...])

    state = obs_ref[...]
    rewards = []
    for t in range(steps):
        high = state.astype(BF16)
        low = (state - high.astype(F32)).astype(BF16)
        inputs[:, t * env : (t + 1) * env] = high
        mixed = mm(state_mix[...], jnp.concatenate([high, low, high], axis=0))
        hidden = jnp.tanh(mixed[:pol]).astype(BF16)
        noise = noise_ref[:, t, :].astype(F32)
        action = jnp.tanh(mm(policy_out_ref[...], hidden)) + NOISE_UNIT * noise
        drift = jnp.tanh(mixed[pol : pol + obs])
        for k in range(feet):
            start = pol + obs * (k + 1)
            touching = contacts_ref[t, k : k + 1, :].astype(F32)
            drift = drift - mixed[start : start + obs] * touching
        for a in range(act):
            drift = drift + act_cols[a] * action[a : a + 1, :]
        state = state + TIME_STEP * drift
        rewards.append(
            0.5
            - jnp.sum(weight_col[...] * state * state, axis=0, keepdims=True) / obs
            - 0.1 * (jnp.sum(action * action, axis=0, keepdims=True) / act)
        )
    inputs[:, rows:] = state.astype(BF16)

    block = 256
    for m in range(hid // block):
        at = slice(m * block, (m + 1) * block)
        pre = mm(critic_in_ref[:, at], inputs[...], TN)
        first[at, :] = jnp.maximum(pre, 0.0).astype(BF16)
    values = jnp.zeros((8, rows + env), F32)
    out_row = jnp.broadcast_to(critic_out_ref[...], (8, hid))
    for m in range(hid // block):
        at = slice(m * block, (m + 1) * block)
        kept = jnp.maximum(mm(middle_t[at, :], first[...]), 0.0).astype(BF16)
        middle[at, :] = kept
        values = values + mm(out_row[:, at], kept)
    value = [values[0:1, t * env : (t + 1) * env] for t in range(steps + 1)]
    target = value[steps]
    weights = [None] * steps
    for t in reversed(range(steps)):
        target = rewards[t] + DISCOUNT * (
            (1.0 - TRACE_DECAY) * value[t + 1] + TRACE_DECAY * target
        )
        targets_ref[t : t + 1, :] = target
        weights[t] = loss_scale * (value[t] - target)
    for t in range(steps):
        lanes = slice(t * env, (t + 1) * env)
        scaled = out_col[...] * weights[t]
        delta[:, lanes] = jnp.where(middle[:, lanes] > 0, scaled, 0.0).astype(BF16)

    per = block // (cores * depth)
    for m in range(hid // block):
        part = mm(first[m * block : (m + 1) * block, :rows], delta[...], NT)
        for i in range(per):
            slot = slot_ref[lax.rem(m * per + i - here + ring, ring)]
            for c in range(cores):
                piece = part[(i * cores + c) * depth : (i * cores + c + 1) * depth]
                grad_ref[lax.rem(core + c, cores), slot] = piece

    for m in range(hid // block):
        at = slice(m * block, (m + 1) * block)
        back = mm(critic_middle_ref[at, :], delta[...])
        first_delta[at, :] = jnp.where(first[at, :rows] > 0, back, 0.0).astype(BF16)
    small_ref[...] = jnp.zeros_like(small_ref)
    small_ref[:obs, :] = mm(inputs[:, :rows], first_delta[...], NT)
    weight_row = jnp.concatenate(weights, axis=1)
    weight_high = weight_row.astype(BF16)
    weight_low = (weight_row - weight_high.astype(F32)).astype(BF16)
    both = mm(jnp.concatenate([weight_high, weight_low], axis=0), middle[:, :rows], NT)
    small_ref[obs : obs + 1, :] = both[0:1] + both[1:2]


def local_window(args, devices, orders, small_rows):
    (first_obs, dyn_state, dyn_act, contact_gain, reward_weight, contacts, action_noise,
     policy_in, policy_out, critic_in, critic_middle, critic_out) = args
    obs, env = first_obs.shape
    steps, feet = contacts.shape[:2]
    hid = critic_middle.shape[0]
    pol = policy_out.shape[1]
    rows = steps * env
    act = dyn_act.shape[1]
    loss_scale = math.sqrt(hid) / (rows * devices)
    depth = hid // devices
    ring = devices // CORES
    slots = np.zeros((ring,), np.int32)
    for slot, offset in enumerate(sum(orders, [])):
        slots[offset % ring] = slot
    vmem = pl.BlockSpec(memory_space=pltpu.VMEM)
    smem = pl.BlockSpec(memory_space=pltpu.SMEM)
    return pl.pallas_call(
        functools.partial(window_kernel, loss_scale, [len(o) for o in orders]),
        in_specs=[smem] + [vmem] * 12,
        out_specs=[vmem] * 3,
        out_shape=[
            jax.ShapeDtypeStruct((steps, env), F32),
            jax.ShapeDtypeStruct((small_rows, hid), F32),
            jax.ShapeDtypeStruct((CORES, ring, depth, hid), F32),
        ],
        scratch_shapes=[
            pltpu.VMEM((pol + obs * (feet + 1), 3 * obs), BF16),
            pltpu.VMEM((obs, rows + env), BF16),
            pltpu.VMEM((hid, rows + env), BF16),
            pltpu.VMEM((hid, rows + env), BF16),
            pltpu.VMEM((hid, rows), BF16),
            pltpu.VMEM((hid, rows), BF16),
            pltpu.VMEM((hid, hid), BF16),
            pltpu.VMEM((hid, env), F32),
            pltpu.VMEM((act, obs, env), F32),
            pltpu.VMEM((obs, env), F32),
        ],
        compiler_params=pltpu.CompilerParams(vmem_limit_bytes=60000 * 1024),
    )(
        jnp.asarray(slots), first_obs, dyn_state, dyn_act.T, contact_gain, reward_weight[None, :],
        contacts, action_noise.transpose(1, 0, 2), policy_in.T, policy_out, critic_in,
        critic_middle, critic_out[None, :]
    )


def per_device(*args):
    devices = lax.axis_size("env")
    ring = devices // CORES
    index = lax.axis_index("env")
    obs = args[0].shape[0]
    hid = args[10].shape[0]
    depth = hid // devices

    split = CORES * 2**LEVELS
    small_rows = 8 * split
    orders = message_orders(ring)
    targets, small, grad = local_window(args, devices, orders, small_rows)

    def shift(x, d):
        pairs = [
            (z * CORES + c, (z + d) % ring * CORES + c) for z in range(ring) for c in range(CORES)
        ]
        return lax.ppermute(x, "env", pairs)

    def swap(x, bit):
        return lax.ppermute(x, "env", [(e, e ^ bit) for e in range(devices)])

    def halves(x, bit):
        half = x.shape[0] // 2
        upper = (index // bit) % 2 == 1
        return jnp.where(upper, x[half:], x[:half]), jnp.where(upper, x[:half], x[half:])

    def joined(mine, other, bit):
        upper = (index // bit) % 2 == 1
        return jnp.concatenate(
            [jnp.where(upper, other, mine), jnp.where(upper, mine, other)], axis=0
        )

    mine, yours = grad[0], grad[1]
    kept, given = halves(small, 1)
    got, other = lax.optimization_barrier((swap(yours, 1), swap(given, 1)))
    total = mine + got
    small = kept + other
    bounds = np.cumsum([0] + [len(o) for o in orders])
    pieces = [total[a:b].reshape(-1, hid) for a, b in zip(bounds[:-1], bounds[1:])]

    for level in range(LEVELS):
        d = 2**level
        kept, given = halves(small, CORES * d)
        right, left, other = lax.optimization_barrier(
            (shift(pieces[2 * level], d), shift(pieces[2 * level + 1], -d), swap(given, CORES * d))
        )
        small = kept + other
        at = 0
        for later in range(level + 1, LEVELS):
            size = pieces[2 * later].shape[0]
            pieces[2 * later] = pieces[2 * later] + right[at : at + size]
            pieces[2 * later + 1] = pieces[2 * later + 1] + left[at : at + size]
            at += size
        right, left = right[at:], left[at:]
        size = right.shape[0]
        pads = pieces[-1].shape[0] - size
        skip = size - depth
        pieces[-1] = (
            pieces[-1]
            + jnp.pad(right, ((0, pads), (0, 0)))
            + jnp.pad(left, ((skip, pads - skip), (0, 0)))
        )

    d = 2**LEVELS
    hops = ring // (2 * d)
    own = small
    sums = {o: pieces[-1][k * depth : (k + 1) * depth] for k, o in enumerate(orders[-1])}
    right = jnp.concatenate([sums[hops * d], own], axis=0)
    left = jnp.concatenate([sums[-(hops - 1) * d], own], axis=0)
    for k in range(1, hops + 1):
        right = shift(right, d)
        if k < hops:
            left = shift(left, -d)
        right, left = lax.optimization_barrier((right, left))
        if k < hops:
            right = right + jnp.concatenate([sums[(hops - k) * d], own], axis=0)
        if k < hops - 1:
            left = left + jnp.concatenate([sums[-(hops - 1 - k) * d], own], axis=0)
    last = right + left
    grad_middle = last[:depth] + sums[0]
    small = last[depth:] + own
    for level in reversed(range(LEVELS)):
        bit = CORES * 2**level
        small = joined(small, swap(small, bit), bit)
    small = joined(small, swap(small, 1), 1)
    return targets, grad_middle, small[:obs], small[obs]


def solution(mesh):
    split = ("parts", "env")
    return jax.shard_map(
        per_device,
        mesh=mesh,
        in_specs=(
            P(None, split),
            P(),
            P(),
            P(),
            P(),
            P(None, None, split),
            P(None, None, split),
            P(),
            P(),
            P(),
            P(),
            P(),
        ),
        out_specs=(P(None, split), P(split, None), P("parts", None), P("parts")),
        check_vma=False,
    )
```

```python
import functools
import math

import jax
import jax.numpy as jnp
import numpy as np
from jax import lax
from jax.experimental import pallas as pl
from jax.experimental.pallas import tpu as pltpu
from jax.sharding import PartitionSpec as P


TIME_STEP = 0.05
NOISE_UNIT = 0.3 / 32768.0
DISCOUNT = 0.99
TRACE_DECAY = 0.95
LEVELS = 2
CORES = 2

F32 = jnp.float32
BF16 = jnp.bfloat16
NT = (((1,), (1,)), ((), ()))
TN = (((0,), (0,)), ((), ()))


def mm(a, b, dims=(((1,), (0,)), ((), ()))):
    return lax.dot_general(a, b, dims, preferred_element_type=F32)


def message_orders(ring):
    d = 2**LEVELS
    half = ring // 2
    behind = [-o for o in range(d, half + 1, d)]
    ahead = list(range(half, 0, -d))
    orders = [behind[:-1] + ahead + [0]]
    for level in reversed(range(LEVELS)):
        d = 2**level
        right, left = [o + d for o in behind], [o - d for o in ahead]
        orders = [right, left] + orders
        behind, ahead = right + behind, left + ahead
    return orders


def column(row, lanes):
    return jnp.transpose(jnp.broadcast_to(row, (lanes, row.shape[1])))


def spread_gradient(slot_ref, first, delta, odd, mine_ref, yours_ref):
    cores = CORES
    count, depth, _ = mine_ref.shape
    rows = delta.shape[1]
    index = lax.axis_index("env")
    here, core = index // cores, lax.rem(index, cores)
    parity = lax.rem(here + odd, 2)
    size = cores * depth
    per = 256 // size
    for m in range(count // per):
        owners = [2 * (m * per + i) + parity for i in range(per)]
        left = jnp.concatenate(
            [first[pl.ds(pl.multiple_of(o * size, size), size), :rows] for o in owners], axis=0
        )
        part = mm(left, delta[...], NT)
        for i, owner in enumerate(owners):
            slot = slot_ref[lax.rem(owner - here + 2 * count, 2 * count)]
            low = part[i * size : i * size + depth]
            high = part[i * size + depth : (i + 1) * size]
            mine_ref[slot] = jnp.where(core == 0, low, high)
            yours_ref[slot] = jnp.where(core == 0, high, low)


def window_kernel(
    loss_scale,
    slot_ref,
    obs_ref,
    dyn_state_ref,
    dyn_act_ref,
    gain_ref,
    reward_weight_ref,
    contacts_ref,
    noise_ref,
    policy_in_ref,
    policy_out_ref,
    critic_in_ref,
    critic_middle_ref,
    critic_out_ref,
    targets_ref,
    inputs,
    first,
    middle,
    delta,
    weight_rows,
    mine_ref,
    yours_ref,
    state_mix,
    middle_copy,
    middle_t,
    out_col,
    act_cols,
    weight_col,
    arrived,
):
    fetch = pltpu.make_async_copy(critic_middle_ref, middle_copy, arrived)
    fetch.start()
    obs, env = obs_ref.shape
    steps, feet, _ = contacts_ref.shape
    act = dyn_act_ref.shape[0]
    pol = policy_out_ref.shape[1]
    hid = critic_middle_ref.shape[0]
    rows = steps * env
    mixing = jnp.concatenate(
        [jnp.transpose(policy_in_ref[...].astype(F32)), dyn_state_ref[...]]
        + [gain_ref[k] for k in range(feet)],
        axis=0,
    )
    top = mixing.astype(BF16).astype(F32)
    state_mix[...] = jnp.concatenate([top, top, mixing - top], axis=1).astype(BF16)
    for a in range(act):
        act_cols[a] = column(dyn_act_ref[a : a + 1, :], env)
    weight_col[...] = column(reward_weight_ref[...], env)
    heads = critic_out_ref[...].astype(F32)
    for j in range(hid // env):
        out_col[j * env : (j + 1) * env, :] = column(heads[j : j + 1, :], env)

    state = obs_ref[...]
    rewards = []
    for t in range(steps):
        high = state.astype(BF16)
        low = (state - high.astype(F32)).astype(BF16)
        inputs[:, t * env : (t + 1) * env] = high
        mixed = mm(state_mix[...], jnp.concatenate([high, low, high], axis=0))
        hidden = jnp.tanh(mixed[:pol]).astype(BF16)
        noise = noise_ref[:, t, :].astype(F32)
        action = jnp.tanh(mm(policy_out_ref[...], hidden)) + NOISE_UNIT * noise
        drift = jnp.tanh(mixed[pol : pol + obs])
        for k in range(feet):
            start = pol + obs * (k + 1)
            touching = contacts_ref[t, k : k + 1, :].astype(F32)
            drift = drift - mixed[start : start + obs] * touching
        for a in range(act):
            drift = drift + act_cols[a] * action[a : a + 1, :]
        state = state + TIME_STEP * drift
        rewards.append(
            0.5
            - jnp.sum(weight_col[...] * state * state, axis=0, keepdims=True) / obs
            - 0.1 * (jnp.sum(action * action, axis=0, keepdims=True) / act)
        )
    inputs[:, rows:] = state.astype(BF16)
    fetch.wait()
    middle_t[...] = jnp.transpose(middle_copy[...])

    block = 256
    for m in range(hid // block):
        at = slice(m * block, (m + 1) * block)
        pre = mm(critic_in_ref[:, at], inputs[...], TN)
        first[at, :] = jnp.maximum(pre, 0.0).astype(BF16)
    values = jnp.zeros((8, rows + env), F32)
    out_row = jnp.concatenate([heads[j : j + 1, :] for j in range(hid // env)], axis=1)
    out_row = jnp.broadcast_to(out_row, (8, hid)).astype(BF16)
    for m in range(hid // block):
        at = slice(m * block, (m + 1) * block)
        kept = jnp.maximum(mm(middle_t[at, :], first[...]), 0.0).astype(BF16)
        middle[at, :] = kept
        values = values + mm(out_row[:, at], kept)
    value = [values[0:1, t * env : (t + 1) * env] for t in range(steps + 1)]
    target = value[steps]
    weights = [None] * steps
    for t in reversed(range(steps)):
        target = rewards[t] + DISCOUNT * (
            (1.0 - TRACE_DECAY) * value[t + 1] + TRACE_DECAY * target
        )
        targets_ref[t : t + 1, :] = target
        weights[t] = loss_scale * (value[t] - target)
        weight_rows[t : t + 1, :] = weights[t]
    for t in range(steps):
        lanes = slice(t * env, (t + 1) * env)
        scaled = out_col[...] * weights[t]
        delta[:, lanes] = jnp.where(middle[:, lanes] > 0, scaled, 0.0).astype(BF16)

    spread_gradient(slot_ref, first, delta, 1, mine_ref, yours_ref)


def even_kernel(slot_ref, first, delta, mine_ref, yours_ref):
    spread_gradient(slot_ref, first, delta, 0, mine_ref, yours_ref)


def back_kernel(
    critic_middle_ref, inputs, first, middle, delta, weight_rows, small_ref, first_delta
):
    obs = inputs.shape[0]
    hid, rows = delta.shape
    steps = weight_rows.shape[0]
    block = 256
    for m in range(hid // block):
        at = slice(m * block, (m + 1) * block)
        back = mm(critic_middle_ref[at, :], delta[...])
        first_delta[at, :] = jnp.where(first[at, :rows] > 0, back, 0.0).astype(BF16)
    small_ref[...] = jnp.zeros_like(small_ref)
    small_ref[:obs, :] = mm(inputs[:, :rows], first_delta[...], NT)
    weight_row = jnp.concatenate([weight_rows[t : t + 1, :] for t in range(steps)], axis=1)
    weight_high = weight_row.astype(BF16)
    weight_low = (weight_row - weight_high.astype(F32)).astype(BF16)
    both = mm(jnp.concatenate([weight_high, weight_low], axis=0), middle[:, :rows], NT)
    small_ref[obs : obs + 1, :] = both[0:1] + both[1:2]


def local_window(args, devices, orders):
    (first_obs, dyn_state, dyn_act, contact_gain, reward_weight, contacts, action_noise,
     policy_in, policy_out, critic_in, critic_middle, critic_out) = args
    obs, env = first_obs.shape
    steps, feet = contacts.shape[:2]
    hid = critic_middle.shape[0]
    pol = policy_out.shape[1]
    rows = steps * env
    act = dyn_act.shape[1]
    loss_scale = math.sqrt(hid) / (rows * devices)
    depth = hid // devices
    ring = devices // CORES
    half = ring // 2
    slots = np.zeros((ring,), np.int32)
    for slot, offset in enumerate(sum(orders, [])):
        slots[offset % ring] = slot % half
    slots = jnp.asarray(slots)
    vmem = pl.BlockSpec(memory_space=pltpu.VMEM)
    smem = pl.BlockSpec(memory_space=pltpu.SMEM)
    anywhere = pl.BlockSpec(memory_space=pl.ANY)
    sent = pltpu.VMEM((half, depth, hid), F32)

    def far(x):
        return pltpu.with_memory_space_constraint(x, pltpu.MemorySpace.HBM)

    targets, inputs, first, middle, delta, weight_rows, *odd = pl.pallas_call(
        functools.partial(window_kernel, loss_scale),
        in_specs=[smem] + [vmem] * 10 + [anywhere, vmem],
        out_specs=[vmem] * 8,
        out_shape=[
            jax.ShapeDtypeStruct((steps, env), F32),
            pltpu.VMEM((obs, rows + env), BF16),
            pltpu.VMEM((hid, rows + env), BF16),
            pltpu.VMEM((hid, rows + env), BF16),
            pltpu.VMEM((hid, rows), BF16),
            pltpu.VMEM((steps, env), F32),
            sent,
            sent,
        ],
        scratch_shapes=[
            pltpu.VMEM((pol + obs * (feet + 1), 3 * obs), BF16),
            pltpu.VMEM((hid, hid), BF16),
            pltpu.VMEM((hid, hid), BF16),
            pltpu.VMEM((hid, env), F32),
            pltpu.VMEM((act, obs, env), F32),
            pltpu.VMEM((obs, env), F32),
            pltpu.SemaphoreType.DMA(()),
        ],
        compiler_params=pltpu.CompilerParams(vmem_limit_bytes=24 * 2**20),
    )(
        *(
            far(x)
            for x in (
                slots, first_obs, dyn_state, dyn_act.T, contact_gain, reward_weight[None, :],
                contacts, action_noise.transpose(1, 0, 2), policy_in.T, policy_out, critic_in,
                critic_middle, critic_out.reshape(-1, env),
            )
        )
    )

    even = pl.pallas_call(
        even_kernel,
        in_specs=[smem, vmem, vmem],
        out_specs=[vmem] * 2,
        out_shape=[sent] * 2,
        compiler_params=pltpu.CompilerParams(vmem_limit_bytes=8 * 2**20),
        cost_estimate=pl.CostEstimate(flops=rows * hid * hid, bytes_accessed=0, transcendentals=0),
    )(far(slots), first, delta)

    def small_gradients(after, small_rows):
        tied = lax.optimization_barrier((weight_rows, after))
        small = pl.pallas_call(
            back_kernel,
            in_specs=[vmem] * 6,
            out_specs=vmem,
            out_shape=pltpu.VMEM((small_rows, hid), F32),
            scratch_shapes=[pltpu.VMEM((hid, rows), BF16)],
            compiler_params=pltpu.CompilerParams(vmem_limit_bytes=12 * 2**20),
            cost_estimate=pl.CostEstimate(
                flops=2 * rows * hid * (hid + 2 * obs), bytes_accessed=0, transcendentals=0
            ),
        )(critic_middle, inputs, first, middle, delta, tied[0])
        return small, tied[1]

    return targets, odd, even, small_gradients


def reduced_window(*args):
    devices = lax.axis_size("env")
    ring = devices // CORES
    index = lax.axis_index("env")
    obs = args[0].shape[0]
    hid = args[10].shape[0]
    depth = hid // devices
    small_rows = 8 * CORES * 2**LEVELS
    orders = message_orders(ring)

    bits = [2**k for k in range(LEVELS + 1)]
    held = lax.optimization_barrier((args[0], *(lax.bitwise_and(index, b) != 0 for b in bits)))
    args = (held[0],) + args[1:]
    flags = dict(zip(bits, held[1:]))
    targets, odd, even, small_gradients = local_window(args, devices, orders)

    def shift(x, d):
        pairs = [
            (z * CORES + c, (z + d) % ring * CORES + c) for z in range(ring) for c in range(CORES)
        ]
        return lax.ppermute(x, "env", pairs)

    def swap(x, mask):
        return lax.ppermute(x, "env", [(e, e ^ mask) for e in range(devices)])

    def halves(x, bit):
        half = x.shape[0] // 2
        low, high = x[:half], x[half:]
        return jnp.where(flags[bit], high, low), jnp.where(flags[bit], low, high)

    def joined(mine, other, bit):
        low, high = jnp.where(flags[bit], other, mine), jnp.where(flags[bit], mine, other)
        return jnp.concatenate([low, high], axis=0)

    sizes = [len(o) for o in orders]
    right, left = sizes[0], sizes[0] + sizes[1]
    total = odd[0] + swap(odd[1], 1)
    given = swap(even[1], 1)
    small, total = small_gradients(total, small_rows)
    messages = [total[:right].reshape(-1, hid), total[right:left].reshape(-1, hid)]
    for level in range(LEVELS):
        d = 2**level
        bit = CORES * d
        if level == 0:
            right = shift(messages[0], d)
            left = shift(messages[1], -d)
            right, left, given = lax.optimization_barrier((right, left, given))
            total = (even[0] + given).reshape(-1, hid)
            bounds = np.cumsum([0] + [s * depth for s in sizes[2:]])
            later = [total[a:b] for a, b in zip(bounds[:-1], bounds[1:])]
            kept, given = halves(small, 1)
            small = kept + swap(given, 1)
            kept, given = halves(small, bit)
            small = kept + swap(given, bit)
        else:
            kept, given = halves(small, bit)
            right, left, given = lax.optimization_barrier(
                (shift(messages[0], d), shift(messages[1], -d), swap(given, bit))
            )
            small = kept + given
        at = 0
        for k in range(0, len(later) - 1, 2):
            part = later[k].shape[0]
            later[k] = later[k] + right[at : at + part]
            later[k + 1] = later[k + 1] + left[at : at + part]
            at += part
        right, left = right[at:], left[at:]
        size = right.shape[0]
        pads = later[-1].shape[0] - size
        skip = size - depth
        later[-1] = (
            later[-1]
            + jnp.pad(right, ((0, pads), (0, 0)))
            + jnp.pad(left, ((skip, pads - skip), (0, 0)))
        )
        messages, later = later[:2], later[2:]

    (rest,) = messages
    d = 2**LEVELS
    hops = ring // (2 * d)
    own = small
    sums = {o: rest[k * depth : (k + 1) * depth] for k, o in enumerate(orders[-1])}
    right = jnp.concatenate([sums[hops * d], own], axis=0)
    left = jnp.concatenate([sums[-(hops - 1) * d], own], axis=0)
    for k in range(1, hops + 1):
        right = shift(right, d)
        if k < hops:
            left = shift(left, -d)
        right, left = lax.optimization_barrier((right, left))
        if k < hops:
            right = right + jnp.concatenate([sums[(hops - k) * d], own], axis=0)
        if k < hops - 1:
            left = left + jnp.concatenate([sums[-(hops - 1 - k) * d], own], axis=0)
    grad_middle = right[:depth] + left[:depth] + sums[0]
    small = right[depth:] + left[depth:] + own

    masks = range(1, 2**LEVELS)
    got = [small] + list(lax.optimization_barrier(tuple(swap(small, CORES * m) for m in masks)))
    for level in reversed(range(LEVELS)):
        got = [joined(got[m], got[m + 2**level], CORES * 2**level) for m in range(2**level)]
    small = joined(got[0], swap(got[0], 1), 1)
    return targets, grad_middle, small[:obs], small[obs]


def solution(mesh):
    split = ("parts", "env")
    return jax.shard_map(
        reduced_window,
        mesh=mesh,
        in_specs=(
            P(None, split),
            P(),
            P(),
            P(),
            P(),
            P(None, None, split),
            P(None, None, split),
            P(),
            P(),
            P(),
            P(),
            P(),
        ),
        out_specs=(P(None, split), P(split, None), P("parts", None), P("parts")),
        check_vma=False,
    )
```

```python
import functools
import math

import jax
import jax.numpy as jnp
from jax import lax
from jax.experimental import pallas as pl
from jax.experimental.pallas import tpu as pltpu
from jax.sharding import PartitionSpec as P


TIME_STEP = 0.05
NOISE_UNIT = 0.3 / 32768.0
DISCOUNT = 0.99
TRACE_DECAY = 0.95
LEVELS = 2
CORES = 2

F32 = jnp.float32
BF16 = jnp.bfloat16
NT = (((1,), (1,)), ((), ()))
TN = (((0,), (0,)), ((), ()))


def mm(a, b, dims=(((1,), (0,)), ((), ()))):
    return lax.dot_general(a, b, dims, preferred_element_type=F32)


def distances(ring):
    far = ring // 2
    return [*range(far, 0, -4), *range(far - 2, 0, -4)], [*range(far - 1, 0, -4)], [*range(far - 3, 0, -4)]


def column(row, lanes):
    return jnp.transpose(jnp.broadcast_to(row, (lanes, row.shape[1])))


def owned_rows(first, delta, owners, size):
    rows = delta.shape[1]
    left = [first[pl.ds(pl.multiple_of(o * size, size), size), :rows] for o in owners]
    return mm(jnp.concatenate(left, axis=0), delta[...], NT)


def spread_gradient(ring, away, first, delta, mine_ref, yours_ref):
    size = mine_ref.shape[0] // len(away)
    index = lax.axis_index("env")
    here, core = index // CORES, lax.rem(index, CORES)
    side = 1 - 2 * core
    for ref, way, serves in ((mine_ref, side, core == 0), (yours_ref, -side, core == 1)):
        part = owned_rows(first, delta, [lax.rem(here + way * o + ring, ring) for o in away], size)
        for i, o in enumerate(away):
            piece = part[i * size : (i + 1) * size]
            if 2 * o == ring:
                piece = jnp.where(serves, piece, 0.0)
            ref[i * size : (i + 1) * size] = piece


def window_kernel(
    loss_scale,
    ring,
    away,
    obs_ref,
    dyn_state_ref,
    dyn_act_ref,
    gain_ref,
    reward_weight_ref,
    contacts_ref,
    noise_ref,
    policy_in_ref,
    policy_out_ref,
    critic_in_ref,
    critic_middle_ref,
    critic_out_ref,
    targets_ref,
    inputs,
    first,
    middle,
    delta,
    weight_rows,
    mine_ref,
    yours_ref,
    state_mix,
    middle_copy,
    middle_t,
    out_col,
    act_cols,
    weight_col,
    arrived,
):
    fetch = pltpu.make_async_copy(critic_middle_ref, middle_copy, arrived)
    fetch.start()
    obs, env = obs_ref.shape
    steps, feet, _ = contacts_ref.shape
    act = dyn_act_ref.shape[0]
    pol = policy_out_ref.shape[1]
    hid = critic_middle_ref.shape[0]
    rows = steps * env
    mixing = jnp.concatenate(
        [jnp.transpose(policy_in_ref[...].astype(F32)), dyn_state_ref[...]]
        + [gain_ref[k] for k in range(feet)],
        axis=0,
    )
    top = mixing.astype(BF16).astype(F32)
    state_mix[...] = jnp.concatenate([top, top, mixing - top], axis=1).astype(BF16)
    for a in range(act):
        act_cols[a] = column(dyn_act_ref[a : a + 1, :], env)
    weight_col[...] = column(reward_weight_ref[...], env)
    heads = critic_out_ref[...].astype(F32)
    for j in range(hid // env):
        out_col[j * env : (j + 1) * env, :] = column(heads[j : j + 1, :], env)

    state = obs_ref[...]
    rewards = []
    for t in range(steps):
        high = state.astype(BF16)
        low = (state - high.astype(F32)).astype(BF16)
        inputs[:, t * env : (t + 1) * env] = high
        mixed = mm(state_mix[...], jnp.concatenate([high, low, high], axis=0))
        hidden = jnp.tanh(mixed[:pol]).astype(BF16)
        noise = noise_ref[:, t, :].astype(F32)
        action = jnp.tanh(mm(policy_out_ref[...], hidden)) + NOISE_UNIT * noise
        drift = jnp.tanh(mixed[pol : pol + obs])
        for k in range(feet):
            start = pol + obs * (k + 1)
            touching = contacts_ref[t, k : k + 1, :].astype(F32)
            drift = drift - mixed[start : start + obs] * touching
        for a in range(act):
            drift = drift + act_cols[a] * action[a : a + 1, :]
        state = state + TIME_STEP * drift
        rewards.append(
            0.5
            - jnp.sum(weight_col[...] * state * state, axis=0, keepdims=True) / obs
            - 0.1 * (jnp.sum(action * action, axis=0, keepdims=True) / act)
        )
    inputs[:, rows:] = state.astype(BF16)
    fetch.wait()
    middle_t[...] = jnp.transpose(middle_copy[...])

    block = 256
    for m in range(hid // block):
        at = slice(m * block, (m + 1) * block)
        pre = mm(critic_in_ref[:, at], inputs[...], TN)
        first[at, :] = jnp.maximum(pre, 0.0).astype(BF16)
    values = jnp.zeros((8, rows + env), F32)
    out_row = jnp.concatenate([heads[j : j + 1, :] for j in range(hid // env)], axis=1)
    out_row = jnp.broadcast_to(out_row, (8, hid)).astype(BF16)
    for m in range(hid // block):
        at = slice(m * block, (m + 1) * block)
        kept = jnp.maximum(mm(middle_t[at, :], first[...]), 0.0).astype(BF16)
        middle[at, :] = kept
        values = values + mm(out_row[:, at], kept)
    value = [values[0:1, t * env : (t + 1) * env] for t in range(steps + 1)]
    target = value[steps]
    weights = [None] * steps
    for t in reversed(range(steps)):
        target = rewards[t] + DISCOUNT * (
            (1.0 - TRACE_DECAY) * value[t + 1] + TRACE_DECAY * target
        )
        targets_ref[t : t + 1, :] = target
        weights[t] = loss_scale * (value[t] - target)
        weight_rows[t : t + 1, :] = weights[t]
    for t in range(steps):
        lanes = slice(t * env, (t + 1) * env)
        scaled = out_col[...] * weights[t]
        delta[:, lanes] = jnp.where(middle[:, lanes] > 0, scaled, 0.0).astype(BF16)

    spread_gradient(ring, away, first, delta, mine_ref, yours_ref)


def odd_kernel(ring, away, first, delta, mine_ref, yours_ref, own_ref):
    spread_gradient(ring, away, first, delta, mine_ref, yours_ref)
    here = lax.axis_index("env") // CORES
    own_ref[...] = owned_rows(first, delta, [here], own_ref.shape[0])


def back_kernel(
    critic_middle_ref, inputs, first, middle, delta, weight_rows, small_ref, first_delta
):
    obs = inputs.shape[0]
    hid, rows = delta.shape
    steps = weight_rows.shape[0]
    block = 256
    for m in range(hid // block):
        at = slice(m * block, (m + 1) * block)
        back = mm(critic_middle_ref[at, :], delta[...])
        first_delta[at, :] = jnp.where(first[at, :rows] > 0, back, 0.0).astype(BF16)
    small_ref[...] = jnp.zeros_like(small_ref)
    small_ref[:obs, :] = mm(inputs[:, :rows], first_delta[...], NT)
    weight_row = jnp.concatenate([weight_rows[t : t + 1, :] for t in range(steps)], axis=1)
    weight_high = weight_row.astype(BF16)
    weight_low = (weight_row - weight_high.astype(F32)).astype(BF16)
    both = mm(jnp.concatenate([weight_high, weight_low], axis=0), middle[:, :rows], NT)
    small_ref[obs : obs + 1, :] = both[0:1] + both[1:2]


def local_window(args, devices, small_rows):
    (first_obs, dyn_state, dyn_act, contact_gain, reward_weight, contacts, action_noise,
     policy_in, policy_out, critic_in, critic_middle, critic_out) = args
    obs, env = first_obs.shape
    steps, feet = contacts.shape[:2]
    hid = critic_middle.shape[0]
    pol = policy_out.shape[1]
    rows = steps * env
    act = dyn_act.shape[1]
    loss_scale = math.sqrt(hid) / (rows * devices)
    ring = devices // CORES
    size = hid // ring
    even, *odd = distances(ring)
    odd = sum(odd, [])
    vmem = pl.BlockSpec(memory_space=pltpu.VMEM)
    anywhere = pl.BlockSpec(memory_space=pl.ANY)

    def far(x):
        return pltpu.with_memory_space_constraint(x, pltpu.MemorySpace.HBM)

    targets, inputs, first, middle, delta, weight_rows, *near = pl.pallas_call(
        functools.partial(window_kernel, loss_scale, ring, even),
        in_specs=[vmem] * 10 + [anywhere, vmem],
        out_specs=[vmem] * 8,
        out_shape=[
            jax.ShapeDtypeStruct((steps, env), F32),
            pltpu.VMEM((obs, rows + env), BF16),
            pltpu.VMEM((hid, rows + env), BF16),
            pltpu.VMEM((hid, rows + env), BF16),
            pltpu.VMEM((hid, rows), BF16),
            pltpu.VMEM((steps, env), F32),
            pltpu.VMEM((len(even) * size, hid), F32),
            pltpu.VMEM((len(even) * size, hid), F32),
        ],
        scratch_shapes=[
            pltpu.VMEM((pol + obs * (feet + 1), 3 * obs), BF16),
            pltpu.VMEM((hid, hid), BF16),
            pltpu.VMEM((hid, hid), BF16),
            pltpu.VMEM((hid, env), F32),
            pltpu.VMEM((act, obs, env), F32),
            pltpu.VMEM((obs, env), F32),
            pltpu.SemaphoreType.DMA(()),
        ],
        compiler_params=pltpu.CompilerParams(vmem_limit_bytes=24 * 2**20),
    )(
        *(
            far(x)
            for x in (
                first_obs, dyn_state, dyn_act.T, contact_gain, reward_weight[None, :], contacts,
                action_noise.transpose(1, 0, 2), policy_in.T, policy_out, critic_in,
                critic_middle, critic_out.reshape(-1, env),
            )
        )
    )
    small = pl.pallas_call(
        back_kernel,
        in_specs=[vmem] * 6,
        out_specs=vmem,
        out_shape=pltpu.VMEM((small_rows, hid), F32),
        scratch_shapes=[pltpu.VMEM((hid, rows), BF16)],
        compiler_params=pltpu.CompilerParams(vmem_limit_bytes=12 * 2**20),
        cost_estimate=pl.CostEstimate(
            flops=2 * rows * hid * (hid + 2 * obs), bytes_accessed=0, transcendentals=0
        ),
    )(critic_middle, inputs, first, middle, delta, weight_rows)
    other = pl.pallas_call(
        functools.partial(odd_kernel, ring, odd),
        in_specs=[vmem] * 2,
        out_specs=[vmem] * 3,
        out_shape=[
            pltpu.VMEM((len(odd) * size, hid), F32),
            pltpu.VMEM((len(odd) * size, hid), F32),
            pltpu.VMEM((size, hid), F32),
        ],
        compiler_params=pltpu.CompilerParams(vmem_limit_bytes=12 * 2**20),
        cost_estimate=pl.CostEstimate(flops=rows * hid * hid, bytes_accessed=0, transcendentals=0),
    )(first, delta)
    return targets, near, other, small


def reduced_window(*args):
    devices = lax.axis_size("env")
    ring = devices // CORES
    index = lax.axis_index("env")
    obs = args[0].shape[0]
    hid = args[10].shape[0]
    size = hid // ring
    small_rows = 8 * CORES * 2**LEVELS

    bits = [2**k for k in range(LEVELS + 1)]
    held = lax.optimization_barrier((args[0], *(lax.bitwise_and(index, b) != 0 for b in bits)))
    args = (held[0],) + args[1:]
    flags = dict(zip(bits, held[1:]))
    targets, near, other, small = local_window(args, devices, small_rows)

    def onward(x, d):
        pairs = [
            (z * CORES + c, (z + (d if c == 0 else -d)) % ring * CORES + c)
            for z in range(ring)
            for c in range(CORES)
        ]
        return lax.ppermute(x, "env", pairs)

    def swap(x, mask):
        return lax.ppermute(x, "env", [(e, e ^ mask) for e in range(devices)])

    def halves(x, bit):
        half = x.shape[0] // 2
        low, high = x[:half], x[half:]
        return jnp.where(flags[bit], high, low), jnp.where(flags[bit], low, high)

    def joined(mine, other, bit):
        low, high = jnp.where(flags[bit], other, mine), jnp.where(flags[bit], mine, other)
        return jnp.concatenate([low, high], axis=0)

    def folded(x, bit):
        kept, given = halves(x, bit)
        return kept + swap(given, bit)

    got = swap(near[1], 1)
    message = near[0] + got
    got = onward(message, 1)
    rest = other[0] + swap(other[1], 1)
    small = folded(folded(folded(small, 1), CORES), 2 * CORES)
    own = joined(small, swap(small, 1), 1)
    got, rest, own = lax.optimization_barrier((got, rest, own))
    half = rest.shape[0] // 2
    message, kept = rest[:half] + got[:half], rest[half:] + got[half:]
    got, passed = lax.optimization_barrier((onward(message, 2), onward(own, 4)))
    kept = kept + got

    hops = kept.shape[0] // size
    chunk = kept[:size]
    sums = [passed]
    for k in range(1, hops):
        got = onward(jnp.concatenate([chunk, sums[-1] + own], axis=0), 4)
        chunk = got[:size] + kept[k * size : (k + 1) * size]
        sums.append(got[size:])

    side = jnp.where(flags[1], sums[-2], sums[-1])
    small = own + side + swap(side, 1)
    small, _ = halves(small, 1)
    masks = range(1, 2**LEVELS)
    chunk, *parts = lax.optimization_barrier(
        (onward(chunk, 1), *(swap(small, CORES * m) for m in masks))
    )
    parts = [small] + parts
    for level in reversed(range(LEVELS)):
        parts = [joined(parts[m], parts[m + 2**level], CORES * 2**level) for m in range(2**level)]
    small = joined(parts[0], swap(parts[0], 1), 1)
    grad_middle = folded(chunk + other[2], 1)
    return targets, grad_middle, small[:obs], small[obs]


def solution(mesh):
    split = ("parts", "env")
    return jax.shard_map(
        reduced_window,
        mesh=mesh,
        in_specs=(
            P(None, split),
            P(),
            P(),
            P(),
            P(),
            P(None, None, split),
            P(None, None, split),
            P(),
            P(),
            P(),
            P(),
            P(),
        ),
        out_specs=(P(None, split), P(split, None), P("parts", None), P("parts")),
        check_vma=False,
    )
```

```python
import functools
import math

import jax
import jax.numpy as jnp
from jax import lax
from jax.experimental import pallas as pl
from jax.experimental.pallas import tpu as pltpu
from jax.sharding import PartitionSpec as P


TIME_STEP = 0.05
NOISE_UNIT = 0.3 / 32768.0
DISCOUNT = 0.99
TRACE_DECAY = 0.95
LEVELS = 2
CORES = 2

F32 = jnp.float32
BF16 = jnp.bfloat16
NT = (((1,), (1,)), ((), ()))
TN = (((0,), (0,)), ((), ()))


def mm(a, b, dims=(((1,), (0,)), ((), ()))):
    return lax.dot_general(a, b, dims, preferred_element_type=F32)


def distances(ring):
    far = ring // 2
    return [*range(far, 0, -4), *range(far - 2, 0, -4)], [*range(far - 1, 0, -4)], [*range(far - 3, 0, -4)]


def column(row, lanes):
    return jnp.transpose(jnp.broadcast_to(row, (lanes, row.shape[1])))


def owned_rows(first, delta, owners, size):
    rows = delta.shape[1]
    left = [first[pl.ds(pl.multiple_of(o * size, size), size), :rows] for o in owners]
    return mm(jnp.concatenate(left, axis=0), delta[...], NT)


def spread_gradient(ring, away, first, delta, mine_ref, yours_ref):
    size = mine_ref.shape[0] // len(away)
    index = lax.axis_index("env")
    here, core = index // CORES, lax.rem(index, CORES)
    side = 1 - 2 * core
    for ref, way, serves in ((mine_ref, side, core == 0), (yours_ref, -side, core == 1)):
        part = owned_rows(first, delta, [lax.rem(here + way * o + ring, ring) for o in away], size)
        for i, o in enumerate(away):
            piece = part[i * size : (i + 1) * size]
            if 2 * o == ring:
                piece = jnp.where(serves, piece, 0.0)
            ref[i * size : (i + 1) * size] = piece


def window_kernel(
    loss_scale,
    ring,
    away,
    obs_ref,
    dyn_state_ref,
    dyn_act_ref,
    gain_ref,
    reward_weight_ref,
    contacts_ref,
    noise_ref,
    policy_in_ref,
    policy_out_ref,
    critic_in_ref,
    critic_middle_ref,
    critic_out_ref,
    targets_ref,
    inputs,
    first,
    middle,
    delta,
    weight_rows,
    mine_ref,
    yours_ref,
    state_mix,
    middle_copy,
    middle_t,
    out_col,
    act_cols,
    weight_col,
    arrived,
):
    fetch = pltpu.make_async_copy(critic_middle_ref, middle_copy, arrived)
    fetch.start()
    obs, env = obs_ref.shape
    steps, feet, _ = contacts_ref.shape
    act = dyn_act_ref.shape[0]
    pol = policy_out_ref.shape[1]
    hid = critic_middle_ref.shape[0]
    rows = steps * env
    mixing = jnp.concatenate(
        [jnp.transpose(policy_in_ref[...].astype(F32)), dyn_state_ref[...]]
        + [gain_ref[k] for k in range(feet)],
        axis=0,
    )
    top = mixing.astype(BF16).astype(F32)
    state_mix[...] = jnp.concatenate([top, top, mixing - top], axis=1).astype(BF16)
    for a in range(act):
        act_cols[a] = column(dyn_act_ref[a : a + 1, :], env)
    weight_col[...] = column(reward_weight_ref[...], env)
    heads = critic_out_ref[...].astype(F32)
    for j in range(hid // env):
        out_col[j * env : (j + 1) * env, :] = column(heads[j : j + 1, :], env)

    state = obs_ref[...]
    rewards = []
    for t in range(steps):
        high = state.astype(BF16)
        low = (state - high.astype(F32)).astype(BF16)
        inputs[:, t * env : (t + 1) * env] = high
        mixed = mm(state_mix[...], jnp.concatenate([high, low, high], axis=0))
        hidden = jnp.tanh(mixed[:pol]).astype(BF16)
        noise = noise_ref[:, t, :].astype(F32)
        action = jnp.tanh(mm(policy_out_ref[...], hidden)) + NOISE_UNIT * noise
        drift = jnp.tanh(mixed[pol : pol + obs])
        for k in range(feet):
            start = pol + obs * (k + 1)
            touching = contacts_ref[t, k : k + 1, :].astype(F32)
            drift = drift - mixed[start : start + obs] * touching
        for a in range(act):
            drift = drift + act_cols[a] * action[a : a + 1, :]
        state = state + TIME_STEP * drift
        rewards.append(
            0.5
            - jnp.sum(weight_col[...] * state * state, axis=0, keepdims=True) / obs
            - 0.1 * (jnp.sum(action * action, axis=0, keepdims=True) / act)
        )
    inputs[:, rows:] = state.astype(BF16)
    fetch.wait()
    middle_t[...] = jnp.transpose(middle_copy[...])

    block = 256
    for m in range(hid // block):
        at = slice(m * block, (m + 1) * block)
        pre = mm(critic_in_ref[:, at], inputs[...], TN)
        first[at, :] = jnp.maximum(pre, 0.0).astype(BF16)
    values = jnp.zeros((8, rows + env), F32)
    out_row = jnp.concatenate([heads[j : j + 1, :] for j in range(hid // env)], axis=1)
    out_row = jnp.broadcast_to(out_row, (8, hid)).astype(BF16)
    for m in range(hid // block):
        at = slice(m * block, (m + 1) * block)
        kept = jnp.maximum(mm(middle_t[at, :], first[...]), 0.0).astype(BF16)
        middle[at, :] = kept
        values = values + mm(out_row[:, at], kept)
    value = [values[0:1, t * env : (t + 1) * env] for t in range(steps + 1)]
    target = value[steps]
    weights = [None] * steps
    for t in reversed(range(steps)):
        target = rewards[t] + DISCOUNT * (
            (1.0 - TRACE_DECAY) * value[t + 1] + TRACE_DECAY * target
        )
        targets_ref[t : t + 1, :] = target
        weights[t] = loss_scale * (value[t] - target)
        weight_rows[t : t + 1, :] = weights[t]
    for t in range(steps):
        lanes = slice(t * env, (t + 1) * env)
        scaled = out_col[...] * weights[t]
        delta[:, lanes] = jnp.where(middle[:, lanes] > 0, scaled, 0.0).astype(BF16)

    spread_gradient(ring, away, first, delta, mine_ref, yours_ref)


def odd_kernel(ring, away, first, delta, targets, mine_ref, yours_ref, own_ref, targets_ref):
    targets_ref[...] = targets[...]
    spread_gradient(ring, away, first, delta, mine_ref, yours_ref)
    here = lax.axis_index("env") // CORES
    own_ref[...] = owned_rows(first, delta, [here], own_ref.shape[0])


def back_kernel(
    critic_middle_ref, inputs, first, middle, delta, weight_rows, small_ref, first_delta
):
    obs = inputs.shape[0]
    hid, rows = delta.shape
    steps = weight_rows.shape[0]
    block = 256
    for m in range(hid // block):
        at = slice(m * block, (m + 1) * block)
        back = mm(critic_middle_ref[at, :], delta[...])
        first_delta[at, :] = jnp.where(first[at, :rows] > 0, back, 0.0).astype(BF16)
    small_ref[...] = jnp.zeros_like(small_ref)
    small_ref[:obs, :] = mm(inputs[:, :rows], first_delta[...], NT)
    weight_row = jnp.concatenate([weight_rows[t : t + 1, :] for t in range(steps)], axis=1)
    weight_high = weight_row.astype(BF16)
    weight_low = (weight_row - weight_high.astype(F32)).astype(BF16)
    both = mm(jnp.concatenate([weight_high, weight_low], axis=0), middle[:, :rows], NT)
    small_ref[obs : obs + 1, :] = both[0:1] + both[1:2]


def join_kernel(kept, given, mine, yours, grad_middle, grad_in, grad_out):
    grad_middle[...] = kept[...] + given[...]
    behind = lax.rem(lax.axis_index("env"), CORES) == 1
    half = mine.shape[0] // 2
    obs = grad_in.shape[0]
    for k in range(2):
        at = slice(k * half, (k + 1) * half)
        for c, same in enumerate((jnp.logical_not(behind), behind)):
            start = (2 * k + c) * half
            part = jnp.where(same, mine[at, :], yours[at, :])
            if start + half <= obs:
                grad_in[start : start + half, :] = part
            elif start <= obs:
                grad_out[...] = part[obs - start : obs - start + 1, :]


def local_window(args, devices, small_rows):
    (first_obs, dyn_state, dyn_act, contact_gain, reward_weight, contacts, action_noise,
     policy_in, policy_out, critic_in, critic_middle, critic_out) = args
    obs, env = first_obs.shape
    steps, feet = contacts.shape[:2]
    hid = critic_middle.shape[0]
    pol = policy_out.shape[1]
    rows = steps * env
    act = dyn_act.shape[1]
    loss_scale = math.sqrt(hid) / (rows * devices)
    ring = devices // CORES
    size = hid // ring
    even, *odd = distances(ring)
    odd = sum(odd, [])
    vmem = pl.BlockSpec(memory_space=pltpu.VMEM)
    anywhere = pl.BlockSpec(memory_space=pl.ANY)

    def far(x):
        return pltpu.with_memory_space_constraint(x, pltpu.MemorySpace.HBM)

    targets, inputs, first, middle, delta, weight_rows, *near = pl.pallas_call(
        functools.partial(window_kernel, loss_scale, ring, even),
        in_specs=[vmem] * 10 + [anywhere, vmem],
        out_specs=[vmem] * 8,
        out_shape=[
            pltpu.VMEM((steps, env), F32),
            pltpu.VMEM((obs, rows + env), BF16),
            pltpu.VMEM((hid, rows + env), BF16),
            pltpu.VMEM((hid, rows + env), BF16),
            pltpu.VMEM((hid, rows), BF16),
            pltpu.VMEM((steps, env), F32),
            pltpu.VMEM((len(even) * size, hid), F32),
            pltpu.VMEM((len(even) * size, hid), F32),
        ],
        scratch_shapes=[
            pltpu.VMEM((pol + obs * (feet + 1), 3 * obs), BF16),
            pltpu.VMEM((hid, hid), BF16),
            pltpu.VMEM((hid, hid), BF16),
            pltpu.VMEM((hid, env), F32),
            pltpu.VMEM((act, obs, env), F32),
            pltpu.VMEM((obs, env), F32),
            pltpu.SemaphoreType.DMA(()),
        ],
        compiler_params=pltpu.CompilerParams(vmem_limit_bytes=24 * 2**20),
    )(
        *(
            far(x)
            for x in (
                first_obs, dyn_state, dyn_act.T, contact_gain, reward_weight[None, :], contacts,
                action_noise.transpose(1, 0, 2), policy_in.T, policy_out, critic_in,
                critic_middle, critic_out.reshape(-1, env),
            )
        )
    )
    small = pl.pallas_call(
        back_kernel,
        in_specs=[vmem] * 6,
        out_specs=vmem,
        out_shape=pltpu.VMEM((small_rows, hid), F32),
        scratch_shapes=[pltpu.VMEM((hid, rows), BF16)],
        compiler_params=pltpu.CompilerParams(vmem_limit_bytes=12 * 2**20),
        cost_estimate=pl.CostEstimate(
            flops=2 * rows * hid * (hid + 2 * obs), bytes_accessed=0, transcendentals=0
        ),
    )(critic_middle, inputs, first, middle, delta, weight_rows)
    other = pl.pallas_call(
        functools.partial(odd_kernel, ring, odd),
        in_specs=[vmem] * 3,
        out_specs=[vmem] * 4,
        out_shape=[
            pltpu.VMEM((len(odd) * size, hid), F32),
            pltpu.VMEM((len(odd) * size, hid), F32),
            pltpu.VMEM((size, hid), F32),
            jax.ShapeDtypeStruct((steps, env), F32),
        ],
        compiler_params=pltpu.CompilerParams(vmem_limit_bytes=12 * 2**20),
        cost_estimate=pl.CostEstimate(flops=rows * hid * hid, bytes_accessed=0, transcendentals=0),
    )(first, delta, targets)
    return near, other, small


def reduced_window(*args):
    devices = lax.axis_size("env")
    ring = devices // CORES
    index = lax.axis_index("env")
    obs = args[0].shape[0]
    hid = args[10].shape[0]
    size = hid // ring
    small_rows = 8 * CORES * 2**LEVELS

    chip_and_core = lax.shift_right_logical(index, 1) + index
    marks = (
        lax.bitwise_and(index, 1) != 0,
        lax.bitwise_and(chip_and_core, 1) != 0,
        lax.bitwise_and(index, 2 * CORES) != 0,
    )
    held = lax.optimization_barrier((args[0], *marks))
    args = (held[0],) + args[1:]
    is_behind, is_odd, is_upper = held[1:]
    near, (*other, targets), small = local_window(args, devices, small_rows)

    def onward(x, d):
        pairs = [
            (z * CORES + c, (z + (d if c == 0 else -d)) % ring * CORES + c)
            for z in range(ring)
            for c in range(CORES)
        ]
        return lax.ppermute(x, "env", pairs)

    def swap(x, mask):
        return lax.ppermute(x, "env", [(e, e ^ mask) for e in range(devices)])

    def across(x):
        ahead = [(e, (e + 1 if e % CORES else e - 1) % devices) for e in range(devices)]
        return lax.ppermute(x, "env", ahead)

    def halves(x, upper):
        half = x.shape[0] // 2
        low, high = x[:half], x[half:]
        return jnp.where(upper, high, low), jnp.where(upper, low, high)

    def joined(mine, other, upper):
        low, high = jnp.where(upper, other, mine), jnp.where(upper, mine, other)
        return jnp.concatenate([low, high], axis=0)

    message = near[0] + swap(near[1], 1)
    kept, given = halves(small, is_odd)
    got = onward(message, 1)
    given = swap(given, 1)
    kept, given = halves(kept + given, is_behind)
    given = across(given)
    rest = other[0] + swap(other[1], 1)
    kept, given = halves(kept + given, is_upper)
    small = kept + swap(given, 2 * CORES)
    own = joined(small, swap(small, 1), is_behind)
    got, rest, own = lax.optimization_barrier((got, rest, own))
    half = rest.shape[0] // 2
    message, kept = rest[:half] + got[:half], rest[half:] + got[half:]
    got, passed = lax.optimization_barrier((onward(message, 2), onward(own, 4)))
    kept = kept + got

    hops = kept.shape[0] // size
    chunk = kept[:size]
    sums = [passed]
    for k in range(1, hops):
        got = onward(jnp.concatenate([chunk, sums[-1] + own], axis=0), 4)
        chunk = got[:size] + kept[k * size : (k + 1) * size]
        sums.append(got[size:])

    side = jnp.where(is_behind, sums[-2], sums[-1])
    small, _ = halves(own + side + swap(side, 1), is_behind)
    chunk = onward(chunk, 1)
    parts = [small] + [swap(small, CORES * m) for m in range(1, 4)]
    chunk, *parts = lax.optimization_barrier((chunk, *parts))
    mine = joined(
        joined(parts[0], parts[2], is_upper), joined(parts[1], parts[3], is_upper), is_odd
    )
    kept, given = halves(chunk + other[2], is_behind)
    vmem = pl.BlockSpec(memory_space=pltpu.VMEM)
    grad_middle, grad_in, grad_out = pl.pallas_call(
        join_kernel,
        in_specs=[vmem] * 4,
        out_specs=[vmem] * 3,
        out_shape=[
            jax.ShapeDtypeStruct(kept.shape, F32),
            jax.ShapeDtypeStruct((obs, hid), F32),
            jax.ShapeDtypeStruct((1, hid), F32),
        ],
        compiler_params=pltpu.CompilerParams(vmem_limit_bytes=4 * 2**20),
    )(kept, swap(given, 1), mine, swap(mine, 1))
    return targets, grad_middle, grad_in, grad_out[0]


def solution(mesh):
    split = ("parts", "env")
    return jax.shard_map(
        reduced_window,
        mesh=mesh,
        in_specs=(
            P(None, split),
            P(),
            P(),
            P(),
            P(),
            P(None, None, split),
            P(None, None, split),
            P(),
            P(),
            P(),
            P(),
            P(),
        ),
        out_specs=(P(None, split), P(split, None), P("parts", None), P("parts")),
        check_vma=False,
    )
```
